128 devices in a mesh: grp: 4 (over y_hi, core), dev: 32 (over x, z, y_lo).
Axes of the slice: x: 4, y: 4 (y_hi: 2, y_lo: 2; y = y_hi * 2 + y_lo), z: 4, core: 2. Of those that a mesh axis runs over, the one named last changes fastest.
Arguments:
- embeddings: bfloat16 [32768, 768], P(('grp', 'dev')), may hold values from -6 to 6
- language: int32 [32768], P(('grp', 'dev')), may hold values from 0 to 108
- sentence_group: int32 [32768], P(('grp', 'dev')), may hold values from 0 to 8191
- pair_mask: int32 [109, 109], replicated, may hold values 0 or 1
Outputs:
- gradient: float32 [32768, 768], P(('grp', 'dev'))
The draws below stay inside these ranges and needn't reach their ends.
All inputs are finite; a program needn't handle non-finite values.
Results may differ from the reference program's by a relative error of at most 0.0012.
Values may be sent and summed in bfloat16 or wider, within the bound.
No kernel may reach another device: no remote copies, remote signals or barrier semaphores. Data moves between devices by JAX's collectives and lax.ppermute only.
A program may use at most 256 MiB of HBM per device.

```python
import math
import jax
import jax.numpy as jnp
from jax import lax

D = 768
LANGS = 109
TOKENS = 32768
GROUPS = 8192


def set_ends(entries, key, least, high):
    spot = [jax.random.randint(jax.random.fold_in(key, axis), (), 0, length) for axis, length in enumerate(entries.shape)]
    main_axis = entries.shape.index(max(entries.shape))
    beside = spot[:main_axis] + [(spot[main_axis] + 1) % entries.shape[main_axis]] + spot[main_axis + 1:]
    return entries.at[tuple(spot)].set(least).at[tuple(beside)].set(high)


def level_of(rng, shape, split, least, top_value):
    gain, own = 1.0, jax.random.fold_in(rng, 6)
    for dim, parts in split:
        draws = jnp.exp(jax.random.uniform(jax.random.fold_in(own, dim), (parts,), jnp.float32, least / len(split), top_value / len(split)))
        gain = gain * jnp.repeat(draws, shape[dim] // parts).reshape([-1 if axis == dim else 1 for axis in range(len(shape))])
    return gain


def centred(stream_key, extent, deviation, reach, split=(), kind=jnp.bfloat16):
    array = jax.random.normal(stream_key, extent, jnp.float32) * deviation
    if len(split) > 0:
        array = level_of(stream_key, extent, split, -0.22, 0.18) * array
    return jnp.clip(array, min=-reach, max=reach).astype(kind)


def setup_inputs(seed: int = 0) -> dict:
    key_list = jax.random.split(jax.random.key(seed), 5)
    embeddings = centred(key_list[0], (TOKENS, D), 1.0, 6.0, ((0, 128),))
    language = set_ends(jax.random.randint(key_list[1], (TOKENS,), 0, LANGS), jax.random.fold_in(key_list[1], 1), 0, LANGS - 1).astype(jnp.int32)
    sentence_group = set_ends(jax.random.randint(key_list[2], (TOKENS,), 0, GROUPS), jax.random.fold_in(key_list[2], 1), 0, GROUPS - 1).astype(jnp.int32)
    pair_mask = set_ends((jax.random.randint(key_list[3], (LANGS, LANGS), 0, 4) < 3).astype(jnp.int32), jax.random.fold_in(key_list[3], 1), 0, 1)
    return {"embeddings": embeddings, "language": language, "sentence_group": sentence_group, "pair_mask": pair_mask}


def reference(embeddings, language, sentence_group, pair_mask):
    scale = 1.0 / math.sqrt(D)
    weight_table = (pair_mask + pair_mask.T).astype(jnp.float32) * 0.5
    lang_onehot = (language[:, None] == jnp.arange(LANGS, dtype=jnp.int32)[None, :]).astype(jnp.float32)
    weight_rows = jnp.dot(lang_onehot, weight_table, precision=lax.Precision.HIGHEST)
    block_rows = math.gcd(TOKENS, 512)
    column_index = jnp.arange(TOKENS, dtype=jnp.int32)

    def one_block(block_index):
        start = (block_index * block_rows).astype(jnp.int32)
        rows = lax.dynamic_slice_in_dim(embeddings, start, block_rows, 0)
        scores = jnp.dot(rows, embeddings.T, preferred_element_type=jnp.float32) * scale
        weight_values = jnp.dot(lax.dynamic_slice_in_dim(weight_rows, start, block_rows, 0), lang_onehot.T, precision=lax.Precision.HIGHEST)
        groups_here = lax.dynamic_slice_in_dim(sentence_group, start, block_rows, 0)
        labels = jnp.where(groups_here[:, None] == sentence_group[None, :], 1.0, -1.0).astype(jnp.float32)
        row_index = start + jnp.arange(block_rows, dtype=jnp.int32)
        offdiag = (row_index[:, None] != column_index[None, :]).astype(jnp.float32)
        coefficient = -weight_values * labels * jax.nn.sigmoid(-labels * scores) * scale * offdiag
        return jnp.dot(coefficient.astype(jnp.bfloat16), embeddings, preferred_element_type=jnp.float32)
    grads = lax.map(one_block, jnp.arange(TOKENS // block_rows, dtype=jnp.int32))
    return grads.reshape(TOKENS, D)
```

```python
import functools
import math

import jax
import jax.numpy as jnp
from jax import lax
from jax.experimental import pallas as pl
from jax.experimental.pallas import tpu as pltpu
from jax.sharding import PartitionSpec as P


AXES = ("grp", "dev")
NT = (((1,), (1,)), ((), ()))
NN = (((1,), (0,)), ((), ()))
TN = (((0,), (0,)), ((), ()))
LANES = 128
LINK_SCALE = 16.0
BLOCK = 256
META = 16


def position(x, z, y, core):
    return ((y >> 1) * 2 + core) * 32 + x * 8 + z * 2 + (y & 1)


def exchange(value, step):
    pairs = []
    for x in range(4):
        for z in range(4):
            for y in range(4):
                for core in range(2):
                    dx, dz, dy, dc = step(core)
                    pairs.append((position(x, z, y, core), position(x ^ dx, z ^ dz, y ^ dy, core ^ dc)))
    return lax.ppermute(value, AXES, pairs)


PLANE = ((1, 0, 0, 0), (0, 1, 0, 0), (3, 0, 0, 0), (0, 3, 0, 0))
LINE = ((0, 0, 1, 0), (0, 0, 3, 0))


def plane_step(stream, k):
    return lambda core: PLANE[(k + 2 * stream + core) % 4]


def line_step(k):
    return lambda core: LINE[(k + core) % 2]


def partner(core):
    return (0, 0, 0, 1)


def meta_rows(language, group, width):
    row = jnp.concatenate([language, group // LANES, group % LANES]).astype(jnp.bfloat16)
    return jnp.pad(row[None], ((0, META - 1), (0, width - row.shape[0])))


def in_vmem(count):
    return [pl.BlockSpec(memory_space=pltpu.VMEM)] * count


def prepare_body(line_ref, table_ref, weight_ref, group_ref):
    lang_ids = lax.broadcasted_iota(jnp.int32, (LANES, BLOCK), 0).astype(jnp.float32)
    for b in range(4):
        meta = line_ref[b * (BLOCK + META) + BLOCK:(b + 1) * (BLOCK + META), :].astype(jnp.float32)
        row = meta[:1]
        onehot = jnp.where(lang_ids == row[:, :BLOCK], 1.0, 0.0).astype(jnp.bfloat16)
        weights = lax.dot_general(onehot, table_ref[...], TN, preferred_element_type=jnp.float32)
        weight_ref[b * BLOCK:(b + 1) * BLOCK, :] = weights.astype(jnp.bfloat16)
        group = row[:, BLOCK:2 * BLOCK] * 128.0 + row[:, 2 * BLOCK:3 * BLOCK]
        group_ref[b * BLOCK:(b + 1) * BLOCK, :] = jnp.broadcast_to(group, (LANES, BLOCK)).T


def prepare(lines, table):
    return pl.pallas_call(
        prepare_body,
        in_specs=in_vmem(2),
        out_specs=in_vmem(2),
        out_shape=[
            jax.ShapeDtypeStruct((4 * BLOCK, LANES), jnp.bfloat16),
            jax.ShapeDtypeStruct((4 * BLOCK, LANES), jnp.float32),
        ],
        cost_estimate=pl.CostEstimate(flops=2 * 4 * BLOCK * LANES * LANES * 16, transcendentals=0, bytes_accessed=0),
        name="prepare",
    )(lines, table)


def pair_body(units, first, blocks, start, tile, scale, diagonal, has_carry, *refs):
    weight_ref, group_ref, line_ref = refs[:3]
    columns = refs[3:3 + len(units)]
    carry_ref = refs[-2] if has_carry else None
    out_ref = refs[-1]
    log_scale = scale * math.log2(math.e)
    lang_ids = lax.broadcasted_iota(jnp.int32, (LANES, LANES), 0).astype(jnp.float32)
    pitch = LANES + META

    def one_block(i, _):
        b = first + i
        rows = line_ref[pl.ds(pl.multiple_of(b * (BLOCK + META), META), BLOCK), :]
        at = pl.ds(pl.multiple_of(b * BLOCK, BLOCK), BLOCK)
        table_rows = weight_ref[at, :]
        groups = group_ref[at, :]
        total = carry_ref[pl.ds(pl.multiple_of((b - start) * BLOCK, BLOCK), BLOCK), :] if has_carry else None
        for side, (data_ref, count) in enumerate(zip(columns, units)):
            for t in range(0, count, tile):
                pieces = range(t, t + tile)
                data = jnp.concatenate([data_ref[p * pitch:p * pitch + LANES, :] for p in pieces], axis=0)
                metas = [data_ref[p * pitch + LANES:(p + 1) * pitch, :].astype(jnp.float32)[:1] for p in pieces]
                scores = lax.dot_general(rows, data, NT, preferred_element_type=jnp.float32)
                onehots = [jnp.where(lang_ids == m[:, :LANES], 1.0, 0.0).astype(jnp.bfloat16) for m in metas]
                weights = lax.dot_general(
                    table_rows, jnp.concatenate(onehots, axis=1), NN, preferred_element_type=jnp.float32
                )
                coefs = []
                for n, (p, m) in enumerate(zip(pieces, metas)):
                    same = groups == m[:, LANES:2 * LANES] * 128.0 + m[:, 2 * LANES:3 * LANES]
                    span = slice(n * LANES, (n + 1) * LANES)
                    power = jnp.exp2(scores[:, span] * jnp.where(same, log_scale, -log_scale))
                    coef = (weights[:, span] * jnp.where(same, -scale, scale)) * (1.0 / (1.0 + power))
                    if diagonal and p == 0:
                        row = lax.broadcasted_iota(jnp.int32, (BLOCK, LANES), 0) + b * BLOCK
                        column = lax.broadcasted_iota(jnp.int32, (BLOCK, LANES), 1) + side * LANES
                        coef = jnp.where(row == column, 0.0, coef)
                    coefs.append(coef.astype(jnp.bfloat16))
                part = lax.dot_general(
                    jnp.concatenate(coefs, axis=1), data, NN, preferred_element_type=jnp.float32
                )
                total = part if total is None else total + part
        out_ref[pl.ds(pl.multiple_of(i * BLOCK, BLOCK), BLOCK), :] = total
        return 0

    if blocks == 1:
        one_block(0, 0)
    else:
        lax.fori_loop(0, blocks, one_block, 0)


def pairs(weight, group, lines, columns, carry, first, blocks, scale, diagonal=False, tile=4):
    width = lines.shape[1]
    units = [c.shape[0] // (LANES + META) for c in columns]
    start, operands = 0, [weight, group, lines, *columns]
    if carry is not None:
        start, value = carry
        operands.append(value)
    rows, total = BLOCK * blocks, LANES * sum(units)
    return pl.pallas_call(
        functools.partial(pair_body, units, first, blocks, start, tile, scale, diagonal, carry is not None),
        in_specs=in_vmem(len(operands)),
        out_specs=in_vmem(1)[0],
        out_shape=jax.ShapeDtypeStruct((rows, width), jnp.float32),
        input_output_aliases={len(operands) - 1: 0} if carry is not None and value.shape[0] == rows else {},
        compiler_params=pltpu.CompilerParams(vmem_limit_bytes=24 << 20),
        cost_estimate=pl.CostEstimate(
            flops=4 * rows * total * width, transcendentals=2 * rows * total, bytes_accessed=0
        ),
        name="pairs",
    )(*operands)


def to_link(value):
    return (value * LINK_SCALE).astype(jnp.float16)


def from_link(value):
    return value.astype(jnp.float32) * (1.0 / LINK_SCALE)


def join(*values):
    return lax.optimization_barrier(jnp.concatenate(values, axis=0))


def gradient(embeddings, language, sentence_group, pair_mask):
    width = embeddings.shape[1]
    scale = 1.0 / math.sqrt(width)
    lang_count = pair_mask.shape[0]
    table = ((pair_mask + pair_mask.T).astype(jnp.float32) * 0.5).astype(jnp.bfloat16)
    table = jnp.pad(table, ((0, LANES - lang_count), (0, LANES - lang_count)))

    streams = []
    for s in range(2):
        half = slice(s * LANES, (s + 1) * LANES)
        streams.append(join(embeddings[half], meta_rows(language[half], sentence_group[half], width)))
    lines = join(embeddings, meta_rows(language, sentence_group, width))
    parts = []
    for k in range(4):
        if k < 2:
            lines = join(lines, exchange(lines, line_step(k)))
        got = [exchange(streams[s], plane_step(s, k)) for s in range(2)]
        if k < 3:
            streams = [join(a, b) for a, b in zip(streams, got)]
        if k > 0:
            parts.append(streams if k == 1 else got)
    weight, group = prepare(lines, table)
    others = [[exchange(join(*part), partner)] for part in parts]

    def step(*rest, **options):
        return pairs(weight, group, lines, *rest, scale=scale, **options)

    total = step(parts[0], None, 0, 4, diagonal=True)
    total = step(others[0], (0, total), 0, 4)
    total = step(parts[1], (0, total), 0, 4)
    total = step(others[1], (0, total), 0, 4)
    late = step(parts[2], (0, total), 2, 2)
    far = step(others[2], (2, late), 3, 1)
    relay = exchange(to_link(far), line_step(0))
    near0 = step(parts[2] + others[2], (0, total), 1, 1)
    back0 = exchange(to_link(near0), line_step(0))
    near1 = step(others[2], (2, late), 2, 1)
    back1 = exchange(to_link(near1 + from_link(relay)), line_step(1))
    final = step(parts[2] + others[2], (0, total), 0, 1)
    return final + from_link(back0) + from_link(back1)


def solution(mesh):
    return jax.shard_map(
        gradient,
        mesh=mesh,
        in_specs=(P(AXES, None), P(AXES), P(AXES), P()),
        out_specs=P(AXES, None),
        check_vma=False,
    )
```

```python
import functools
import math

import jax
import jax.numpy as jnp
from jax import lax
from jax.experimental import pallas as pl
from jax.experimental.pallas import tpu as pltpu
from jax.sharding import PartitionSpec as P


AXES = ("grp", "dev")
NT = (((1,), (1,)), ((), ()))
NN = (((1,), (0,)), ((), ()))
TN = (((0,), (0,)), ((), ()))
LANES = 128
LINK_SCALE = 16.0
BLOCK = 256
META = 16


def position(x, z, y, core):
    return ((y >> 1) * 2 + core) * 32 + x * 8 + z * 2 + (y & 1)


def exchange(value, step):
    pairs = []
    for x in range(4):
        for z in range(4):
            for y in range(4):
                for core in range(2):
                    dx, dz, dy, dc = step(core)
                    pairs.append((position(x, z, y, core), position(x ^ dx, z ^ dz, y ^ dy, core ^ dc)))
    return lax.ppermute(value, AXES, pairs)


PLANE = ((1, 0, 0, 0), (0, 1, 0, 0), (3, 0, 0, 0), (0, 3, 0, 0))
LINE = ((0, 0, 1, 0), (0, 0, 3, 0))


def plane_step(stream, k):
    return lambda core: PLANE[(k + 2 * stream + core) % 4]


def line_step(k):
    return lambda core: LINE[(k + core) % 2]


def partner(core):
    return (0, 0, 0, 1)


def in_vmem(count):
    return [pl.BlockSpec(memory_space=pltpu.VMEM)] * count


def pack_body(rows_ref, language_ref, group_ref, mask_ref, line_ref, first_ref, second_ref, table_ref, square_ref):
    width = rows_ref.shape[1]
    language = language_ref[...].astype(jnp.float32)
    group = group_ref[...]
    digits = [language, (group // LANES).astype(jnp.float32), (group % LANES).astype(jnp.float32)]

    def row_of(values):
        row = jnp.concatenate(values, axis=1)
        if row.shape[1] < width:
            row = jnp.concatenate([row, jnp.zeros((1, width - row.shape[1]), jnp.float32)], axis=1)
        return jnp.broadcast_to(row, (META, width)).astype(jnp.bfloat16)

    count = mask_ref.shape[0]
    square_ref[...] = jnp.zeros_like(square_ref)
    square_ref[:count, :count] = mask_ref[...].astype(jnp.float32)
    square = square_ref[...]
    table_ref[...] = ((square + square.T) * 0.5).astype(jnp.bfloat16)
    line_ref[:BLOCK, :] = rows_ref[...]
    line_ref[BLOCK:, :] = row_of([d[h:h + 1] for d in digits for h in range(2)])
    for h, ref in enumerate((first_ref, second_ref)):
        ref[:LANES, :] = rows_ref[h * LANES:(h + 1) * LANES, :]
        ref[LANES:, :] = row_of([d[h:h + 1] for d in digits])


def pack(embeddings, language, sentence_group, pair_mask):
    width = embeddings.shape[1]
    shapes = [(BLOCK + META, width), (LANES + META, width), (LANES + META, width), (LANES, LANES)]
    return pl.pallas_call(
        pack_body,
        in_specs=in_vmem(4),
        out_specs=in_vmem(4),
        out_shape=[pltpu.VMEM(shape, jnp.bfloat16) for shape in shapes],
        scratch_shapes=[pltpu.VMEM((LANES, LANES), jnp.float32)],
        name="pack",
    )(embeddings, language.reshape(2, LANES), sentence_group.reshape(2, LANES), pair_mask)


def block_of(line_refs, b):
    return line_refs[b].at[:] if len(line_refs) == 2 else line_refs[0].at[b * (BLOCK + META):(b + 1) * (BLOCK + META)]


def lookup_rows(line_refs, table_ref):
    lang_ids = lax.broadcasted_iota(jnp.int32, (LANES, BLOCK), 0).astype(jnp.float32)
    weights, groups = [], []
    for b in range(2):
        row = block_of(line_refs, b)[BLOCK:, :].astype(jnp.float32)[:1]
        onehot = jnp.where(lang_ids == row[:, :BLOCK], 1.0, 0.0).astype(jnp.bfloat16)
        weights.append(lax.dot_general(onehot, table_ref[...], TN, preferred_element_type=jnp.float32))
        group = row[:, BLOCK:2 * BLOCK] * 128.0 + row[:, 2 * BLOCK:3 * BLOCK]
        groups.append(jnp.broadcast_to(group, (LANES, BLOCK)).T)
    return jnp.concatenate(weights, axis=0), jnp.concatenate(groups, axis=0)


def pair_body(units, line_count, first, blocks, tile, scale, diagonal, looked_up, carry_first, *refs):
    if looked_up:
        weight_ref, group_ref, *rest = refs
        out_ref = refs[-1]
    else:
        table_ref, *rest = refs
        out_ref, weight_ref, group_ref = refs[-3:]
        weight_ref[...], group_ref[...] = lookup_rows(rest[:line_count], table_ref)
    line_refs, columns = rest[:line_count], rest[line_count:line_count + len(units)]
    carry_ref = refs[-2] if carry_first is not None else None
    log_scale = scale * math.log2(math.e)
    pitch = LANES + META
    height = blocks * BLOCK
    rows = jnp.concatenate([block_of(line_refs, b)[:BLOCK, :] for b in range(first, first + blocks)], axis=0)
    table_rows = weight_ref[first * BLOCK:first * BLOCK + height, :]
    groups = group_ref[first * BLOCK:first * BLOCK + height, :]
    total = None
    if carry_ref is not None:
        total = carry_ref[carry_first * BLOCK:carry_first * BLOCK + height, :]
    share = tile // len(columns)

    def add_tile(t, total):
        pieces = []
        for side, ref in enumerate(columns):
            for p in range(share):
                at = (t * share + p) * pitch
                pieces.append((side, ref, at if isinstance(at, int) else pl.multiple_of(at, META)))
        data = jnp.concatenate([ref[pl.ds(at, LANES), :] for _, ref, at in pieces], axis=0)
        scores = lax.dot_general(rows, data, NT, preferred_element_type=jnp.float32)
        coefs = []
        for n, (side, ref, at) in enumerate(pieces):
            meta = ref[pl.ds(at + LANES, META), :].astype(jnp.float32)[:1]
            same = groups == meta[:, LANES:2 * LANES] * 128.0 + meta[:, 2 * LANES:3 * LANES]
            power = jnp.exp2(scores[:, n * LANES:(n + 1) * LANES] * jnp.where(same, log_scale, -log_scale))
            index = jnp.broadcast_to(meta[:, :LANES].astype(jnp.int32), (height, LANES))
            weights = jnp.take_along_axis(table_rows, index, axis=1)
            coef = (weights * jnp.where(same, -scale, scale)) * (1.0 / (1.0 + power))
            if diagonal and n % share == 0:
                assert share == units[0]
                row = lax.broadcasted_iota(jnp.int32, (height, LANES), 0)
                column = lax.broadcasted_iota(jnp.int32, (height, LANES), 1) + side * LANES
                coef = jnp.where(row == column, 0.0, coef)
            coefs.append(coef.astype(jnp.bfloat16))
        part = lax.dot_general(jnp.concatenate(coefs, axis=1), data, NN, preferred_element_type=jnp.float32)
        return part if total is None else total + part

    tiles = units[0] // share
    if tiles == 1 or blocks == 1:
        for t in range(tiles):
            total = add_tile(t, total)
        out_ref[...] = total
        return
    out_ref[...] = jnp.zeros((height, rows.shape[1]), jnp.float32) if total is None else total

    def one_tile(t, _):
        out_ref[...] = add_tile(t, out_ref[...])
        return 0

    lax.fori_loop(0, tiles, one_tile, 0)


def pairs(lookup, line, columns, carry, scale, first=0, blocks=2, carry_first=0, diagonal=False, tile=8):
    width = line[0].shape[1]
    looked_up = isinstance(lookup, tuple)
    units = [c.shape[0] // (LANES + META) for c in columns]
    operands = [*lookup, *line, *columns] if looked_up else [lookup, *line, *columns]
    rows, total = BLOCK * blocks, LANES * sum(units)
    aliases = {}
    if carry is not None:
        operands.append(carry)
        aliases = {len(operands) - 1: 0} if carry.shape[0] == rows else {}
    outs = [pltpu.VMEM((rows, width), jnp.float32)]
    if not looked_up:
        outs += [pltpu.VMEM((rows, LANES), jnp.float32)] * 2
    operands = [pltpu.with_memory_space_constraint(value, pltpu.VMEM) for value in operands]
    out = pl.pallas_call(
        functools.partial(
            pair_body, units, len(line), first, blocks, tile, scale, diagonal, looked_up, carry_first if carry is not None else None
        ),
        in_specs=in_vmem(len(operands)),
        out_specs=in_vmem(len(outs)),
        out_shape=outs,
        input_output_aliases=aliases,
        compiler_params=pltpu.CompilerParams(vmem_limit_bytes=8 << 20),
        cost_estimate=pl.CostEstimate(
            flops=4 * rows * total * width, transcendentals=2 * rows * total, bytes_accessed=0
        ),
        name="pairs",
    )(*operands)
    return out[0] if looked_up else out


def to_link(value):
    return (value * LINK_SCALE).astype(jnp.float16)


def from_link(value):
    return value.astype(jnp.float32) * (1.0 / LINK_SCALE)


def join(*values):
    return lax.optimization_barrier(jnp.concatenate(values, axis=0))


def gradient(embeddings, language, sentence_group, pair_mask):
    width = embeddings.shape[1]
    scale = 1.0 / math.sqrt(width)
    line, *streams, table = pack(embeddings, language, sentence_group, pair_mask)
    arrived = []
    for k in range(2):
        got = [exchange(streams[s], plane_step(s, k)) for s in range(2)]
        if k == 0:
            near = [line, exchange(line, line_step(0))]
            far = [exchange(join(*near), line_step(1))]
        for s in range(2):
            streams[s] = join(streams[s], got[s])
    arrived.append(streams)
    arrived.append([exchange(streams[s], plane_step(s, 2)) for s in range(2)])
    for n in range(2):
        arrived.append([exchange(arrived[n][s], plane_step(s, 3)) for s in range(2)])
    others = [[exchange(part[s], partner) for s in range(2)] for part in arrived]

    def step(*rest, **options):
        return pairs(*rest, scale=scale, **options)

    near_sum, *near_lookup = step(table, near, arrived[0], None, diagonal=True)
    near_lookup = tuple(near_lookup)
    near_sum = step(near_lookup, near, others[0], near_sum)
    both = [own + other for own, other in zip(arrived, others)]
    near_sum = step(near_lookup, near, both[1], near_sum)
    far_sum, *far_lookup = step(table, far, both[0], None)
    far_lookup = tuple(far_lookup)
    far_sum = step(far_lookup, far, both[1], far_sum)
    far_sum = step(far_lookup, far, both[2], far_sum)
    far_sum = step(far_lookup, far, arrived[3], far_sum)
    last = step(far_lookup, far, others[3], far_sum, first=1, blocks=1, carry_first=1)
    relay = exchange(to_link(last), line_step(0))
    near0 = step(near_lookup, near, both[2] + both[3], near_sum, first=1, blocks=1, carry_first=1)
    back0 = exchange(to_link(near0), line_step(0))
    near1 = step(far_lookup, far, others[3], far_sum, first=0, blocks=1, carry_first=0)
    back1 = exchange(to_link(near1 + from_link(relay)), line_step(1))
    final = step(near_lookup, near, both[2] + both[3], near_sum, first=0, blocks=1, carry_first=0)
    return final + from_link(back0) + from_link(back1)


def solution(mesh):
    return jax.shard_map(
        gradient,
        mesh=mesh,
        in_specs=(P(AXES, None), P(AXES), P(AXES), P()),
        out_specs=P(AXES, None),
        check_vma=False,
    )
```

```python
import functools
import math

import jax
import jax.numpy as jnp
from jax import lax
from jax.experimental import pallas as pl
from jax.experimental.pallas import tpu as pltpu
from jax.sharding import PartitionSpec as P


AXES = ("grp", "dev")
NT = (((1,), (1,)), ((), ()))
NN = (((1,), (0,)), ((), ()))
TN = (((0,), (0,)), ((), ()))
LANES = 128
LINK_SCALE = 16.0
BLOCK = 256
META = 8


def position(x, z, y, core):
    return ((y >> 1) * 2 + core) * 32 + x * 8 + z * 2 + (y & 1)


def exchange(value, step):
    pairs = []
    for x in range(4):
        for z in range(4):
            for y in range(4):
                for core in range(2):
                    dx, dz, dy, dc = step(core)
                    pairs.append((position(x, z, y, core), position(x ^ dx, z ^ dz, y ^ dy, core ^ dc)))
    return lax.ppermute(value, AXES, pairs)


PLANE = ((1, 0, 0, 0), (0, 1, 0, 0), (3, 0, 0, 0), (0, 3, 0, 0))
LINE = ((0, 0, 1, 0), (0, 0, 3, 0))


def plane_step(stream, k):
    return lambda core: PLANE[(k + 2 * stream + core) % 4]


def line_step(k):
    return lambda core: LINE[(k + core) % 2]


def partner(core):
    return (0, 0, 0, 1)


def in_vmem(count):
    return [pl.BlockSpec(memory_space=pltpu.VMEM)] * count


def pack_body(rows_ref, language_ref, group_ref, mask_ref, line_ref, first_ref, second_ref, table_ref, square_ref):
    width = rows_ref.shape[1]
    language = language_ref[...].astype(jnp.float32)
    group = group_ref[...]
    digits = [language, (group // LANES).astype(jnp.float32), (group % LANES).astype(jnp.float32)]

    def row_of(values):
        row = jnp.concatenate(values, axis=1)
        if row.shape[1] < width:
            row = jnp.concatenate([row, jnp.zeros((1, width - row.shape[1]), jnp.float32)], axis=1)
        return jnp.broadcast_to(row, (META, width)).astype(jnp.bfloat16)

    count = mask_ref.shape[0]
    square_ref[...] = jnp.zeros_like(square_ref)
    square_ref[:count, :count] = mask_ref[...].astype(jnp.float32)
    square = square_ref[...]
    table_ref[...] = ((square + square.T) * 0.5).astype(jnp.bfloat16)
    line_ref[:BLOCK, :] = rows_ref[...]
    line_ref[BLOCK:, :] = row_of([d[h:h + 1] for d in digits for h in range(2)])
    for h, ref in enumerate((first_ref, second_ref)):
        ref[:LANES, :] = rows_ref[h * LANES:(h + 1) * LANES, :]
        ref[LANES:, :] = row_of([d[h:h + 1] for d in digits])


def pack(embeddings, language, sentence_group, pair_mask):
    width = embeddings.shape[1]
    shapes = [(BLOCK + META, width), (LANES + META, width), (LANES + META, width), (LANES, LANES)]
    return pl.pallas_call(
        pack_body,
        in_specs=in_vmem(4),
        out_specs=in_vmem(4),
        out_shape=[pltpu.VMEM(shape, jnp.bfloat16) for shape in shapes],
        scratch_shapes=[pltpu.VMEM((LANES, LANES), jnp.float32)],
        name="pack",
    )(embeddings, language.reshape(2, LANES), sentence_group.reshape(2, LANES), pair_mask)


def block_of(line_refs, b):
    return line_refs[b].at[:] if len(line_refs) == 2 else line_refs[0].at[b * (BLOCK + META):(b + 1) * (BLOCK + META)]


def lookup_rows(line_refs, table_ref):
    lang_ids = lax.broadcasted_iota(jnp.int32, (LANES, BLOCK), 0).astype(jnp.float32)
    weights, groups = [], []
    for b in range(2):
        row = block_of(line_refs, b)[BLOCK:, :].astype(jnp.float32)[:1]
        onehot = jnp.where(lang_ids == row[:, :BLOCK], 1.0, 0.0).astype(jnp.bfloat16)
        weights.append(lax.dot_general(onehot, table_ref[...], TN, preferred_element_type=jnp.float32))
        group = row[:, BLOCK:2 * BLOCK] * 128.0 + row[:, 2 * BLOCK:3 * BLOCK]
        groups.append(jnp.broadcast_to(group, (LANES, BLOCK)).T)
    return jnp.concatenate(weights, axis=0), jnp.concatenate(groups, axis=0)


def pair_body(units, line_count, first, blocks, tile, scale, diagonal, looked_up, carry_first, *refs):
    if looked_up:
        weight_ref, group_ref, *rest = refs
        out_ref = refs[-1]
    else:
        table_ref, *rest = refs
        out_ref, weight_ref, group_ref = refs[-3:]
        weight_ref[...], group_ref[...] = lookup_rows(rest[:line_count], table_ref)
    line_refs, columns = rest[:line_count], rest[line_count:line_count + len(units)]
    carry_ref = refs[-2] if carry_first is not None else None
    log_scale = scale * math.log2(math.e)
    pitch = LANES + META
    height = blocks * BLOCK
    rows = jnp.concatenate([block_of(line_refs, b)[:BLOCK, :] for b in range(first, first + blocks)], axis=0)
    table_rows = weight_ref[first * BLOCK:first * BLOCK + height, :]
    groups = group_ref[first * BLOCK:first * BLOCK + height, :]
    total = None
    if carry_ref is not None:
        total = carry_ref[carry_first * BLOCK:carry_first * BLOCK + height, :]
    share = tile // len(columns)

    def add_tile(t, total):
        pieces = []
        for side, ref in enumerate(columns):
            for p in range(share):
                at = (t * share + p) * pitch
                pieces.append((side, ref, at if isinstance(at, int) else pl.multiple_of(at, META)))
        data = jnp.concatenate([ref[pl.ds(at, LANES), :] for _, ref, at in pieces], axis=0)
        scores = lax.dot_general(rows, data, NT, preferred_element_type=jnp.float32)
        coefs = []
        for n, (side, ref, at) in enumerate(pieces):
            meta = ref[pl.ds(at + LANES, META), :].astype(jnp.float32)[:1]
            same = groups == meta[:, LANES:2 * LANES] * 128.0 + meta[:, 2 * LANES:3 * LANES]
            power = jnp.exp2(scores[:, n * LANES:(n + 1) * LANES] * jnp.where(same, log_scale, -log_scale))
            index = jnp.broadcast_to(meta[:, :LANES].astype(jnp.int32), (height, LANES))
            weights = jnp.take_along_axis(table_rows, index, axis=1)
            coef = (weights * jnp.where(same, -scale, scale)) * (1.0 / (1.0 + power))
            if diagonal and n % share == 0:
                assert share == units[0]
                row = lax.broadcasted_iota(jnp.int32, (height, LANES), 0)
                column = lax.broadcasted_iota(jnp.int32, (height, LANES), 1) + side * LANES
                coef = jnp.where(row == column, 0.0, coef)
            coefs.append(coef.astype(jnp.bfloat16))
        part = lax.dot_general(jnp.concatenate(coefs, axis=1), data, NN, preferred_element_type=jnp.float32)
        return part if total is None else total + part

    tiles = units[0] // share
    if tiles == 1 or blocks == 1:
        for t in range(tiles):
            total = add_tile(t, total)
        out_ref[...] = total
        return
    out_ref[...] = jnp.zeros((height, rows.shape[1]), jnp.float32) if total is None else total

    def one_tile(t, _):
        out_ref[...] = add_tile(t, out_ref[...])
        return 0

    lax.fori_loop(0, tiles, one_tile, 0)


def pairs(lookup, line, columns, carry, scale, first=0, blocks=2, carry_first=0, diagonal=False, tile=8):
    width = line[0].shape[1]
    looked_up = isinstance(lookup, tuple)
    units = [c.shape[0] // (LANES + META) for c in columns]
    operands = [*lookup, *line, *columns] if looked_up else [lookup, *line, *columns]
    rows, total = BLOCK * blocks, LANES * sum(units)
    aliases = {}
    if carry is not None:
        operands.append(carry)
        aliases = {len(operands) - 1: 0} if carry.shape[0] == rows else {}
    outs = [pltpu.VMEM((rows, width), jnp.float32)]
    if not looked_up:
        outs += [pltpu.VMEM((rows, LANES), jnp.float32)] * 2
    operands = [pltpu.with_memory_space_constraint(value, pltpu.VMEM) for value in operands]
    out = pl.pallas_call(
        functools.partial(
            pair_body, units, len(line), first, blocks, tile, scale, diagonal, looked_up, carry_first if carry is not None else None
        ),
        in_specs=in_vmem(len(operands)),
        out_specs=in_vmem(len(outs)),
        out_shape=outs,
        input_output_aliases=aliases,
        compiler_params=pltpu.CompilerParams(vmem_limit_bytes=8 << 20),
        cost_estimate=pl.CostEstimate(
            flops=4 * rows * total * width, transcendentals=2 * rows * total, bytes_accessed=0
        ),
        name="pairs",
    )(*operands)
    return out[0] if looked_up else out


def to_link(value):
    return (value * LINK_SCALE).astype(jnp.float16)


def from_link(value):
    return value.astype(jnp.float32) * (1.0 / LINK_SCALE)


def join(*values):
    return lax.optimization_barrier(jnp.concatenate(values, axis=0))


def gradient(embeddings, language, sentence_group, pair_mask):
    width = embeddings.shape[1]
    scale = 1.0 / math.sqrt(width)
    line, *streams, table = pack(embeddings, language, sentence_group, pair_mask)
    arrived = []
    for k in range(2):
        got = [exchange(streams[s], plane_step(s, k)) for s in range(2)]
        if k == 0:
            near = [line, exchange(line, line_step(0))]
            far = [exchange(join(*near), line_step(1))]
        for s in range(2):
            streams[s] = join(streams[s], got[s])
    arrived.append(streams)
    arrived.append([exchange(streams[s], plane_step(s, 2)) for s in range(2)])
    for n in range(2):
        arrived.append([exchange(arrived[n][s], plane_step(s, 3)) for s in range(2)])
    others = [[exchange(part[s], partner) for s in range(2)] for part in arrived]

    def step(*rest, **options):
        return pairs(*rest, scale=scale, **options)

    near_sum, *near_lookup = step(table, near, arrived[0], None, diagonal=True)
    near_lookup = tuple(near_lookup)
    near_sum = step(near_lookup, near, others[0], near_sum)
    both = [own + other for own, other in zip(arrived, others)]
    near_sum = step(near_lookup, near, both[1], near_sum)
    far_sum, *far_lookup = step(table, far, arrived[0], None)
    far_lookup = tuple(far_lookup)
    far_sum = step(far_lookup, far, others[0], far_sum)
    far_sum = step(far_lookup, far, arrived[1], far_sum)
    far_sum = step(far_lookup, far, others[1], far_sum)
    far_sum = step(far_lookup, far, both[2], far_sum)
    near_part = step(near_lookup, near, both[2], near_sum, first=1, blocks=1, carry_first=1)
    far_sum = step(far_lookup, far, arrived[3], far_sum)
    last = step(far_lookup, far, others[3], far_sum, first=1, blocks=1, carry_first=1)
    relay = exchange(to_link(last), line_step(0))
    near0 = step(near_lookup, near, both[3], near_part, first=1, blocks=1, carry_first=0)
    back0 = exchange(to_link(near0), line_step(0))
    near1 = step(far_lookup, far, others[3], far_sum, first=0, blocks=1, carry_first=0)
    back1 = exchange(to_link(near1 + from_link(relay)), line_step(1))
    final = step(near_lookup, near, both[2] + both[3], near_sum, first=0, blocks=1, carry_first=0)
    return final + from_link(back0) + from_link(back1)


def solution(mesh):
    return jax.shard_map(
        gradient,
        mesh=mesh,
        in_specs=(P(AXES, None), P(AXES), P(AXES), P()),
        out_specs=P(AXES, None),
        check_vma=False,
    )
```
